256 devices in a mesh: section: 16 (over z, y_hi), seq: 16 (over y_lo, x, core).
Axes of the slice: x: 4, y: 4 (y_hi: 2, y_lo: 2; y = y_hi * 2 + y_lo), z: 8, core: 2. Of those that a mesh axis runs over, the one named last changes fastest.
Arguments:
- queries: bfloat16 [14336, 4096], P(('section', 'seq')), may hold values from -200 to 200
- key_vectors: bfloat16 [14336, 4096], P(('section', 'seq')), may hold values from -6 to 6
- value_vectors: bfloat16 [14336, 4096], P(('section', 'seq')), may hold values from -6 to 6
- noise_levels: int32 [16], replicated, may hold values from 0 to 15
- visible: int32 [16, 16], replicated, may hold values 0 or 1
- level_gates: float32 [16, 4096], replicated, may hold values from 0.5 to 2
Outputs:
- attended: bfloat16 [14336, 4096], P(('section', 'seq'))
The draws below stay inside these ranges and needn't reach their ends.
All inputs are finite; a program needn't handle non-finite values.
Results may differ from the reference program's by a relative error of at most 0.0045.
Values may be sent and summed in bfloat16 or wider, within the bound.
No kernel may reach another device: no remote copies, remote signals or barrier semaphores. Data moves between devices by JAX's collectives and lax.ppermute only.
A program may use at most 128 MiB of HBM per device.

```python
import math
import jax
import jax.numpy as jnp
from jax import lax

HEADS = 32
HEAD_DIM = 128
LEVELS = 16
GROUPS = 16
TOKENS = 14336
WIDTH = 4096


def paired_vectors(key):
    key_query = jax.random.fold_in(key, 101)
    key_keys = jax.random.fold_in(key, 202)
    keys_float = jnp.clip(jax.random.normal(key_keys, (TOKENS, WIDTH), jnp.float32), -6.0, 6.0)
    query_float = jnp.clip(2.5 * jax.random.normal(key_query, (TOKENS, WIDTH), jnp.float32), -15.0, 15.0)
    return (query_float, keys_float)


def draw_queries(key, part):
    return paired_vectors(key)[0].astype(jnp.bfloat16)


def draw_key_vectors(key, part):
    return paired_vectors(key)[1].astype(jnp.bfloat16)


def plant(values, key, least, largest):
    place = [jax.random.randint(jax.random.fold_in(key, axis), (), 0, length) for axis, length in enumerate(values.shape)]
    main_axis = values.shape.index(max(values.shape))
    next_to = place[:main_axis] + [(place[main_axis] + 1) % values.shape[main_axis]] + place[main_axis + 1:]
    return values.at[tuple(place)].set(least).at[tuple(next_to)].set(largest)


def steps_of(own_key, dims, shards, least, high):
    factor_of, own = 1.0, jax.random.fold_in(own_key, 6)
    for dim, shards_of in shards:
        draws = jnp.exp(jax.random.uniform(jax.random.fold_in(own, dim), (shards_of,), jnp.float32, least / len(shards), high / len(shards)))
        factor_of = factor_of * jnp.repeat(draws, dims[dim] // shards_of).reshape([-1 if axis == dim else 1 for axis in range(len(dims))])
    return factor_of


def gaussian(own_key, dims, scale, bound, shards=(), held_as=jnp.bfloat16):
    entries = jax.random.normal(own_key, dims, jnp.float32) * scale
    if len(shards) > 0:
        entries = steps_of(own_key, dims, shards, -0.22, 0.18) * entries
    return jnp.clip(entries, min=-bound, max=bound).astype(held_as)


def setup_inputs(seed: int = 0) -> dict:
    splits = jax.random.split(jax.random.key(seed), 7)
    return {
        "queries": draw_queries(jax.random.fold_in(splits[6], 71), 0),
        "key_vectors": draw_key_vectors(jax.random.fold_in(splits[6], 71), 0),
        "value_vectors": gaussian(splits[2], (TOKENS, WIDTH), 1.0, 6.0, ((0, 256),)),
        "noise_levels": plant(jax.random.randint(splits[3], (GROUPS,), 0, LEVELS), jax.random.fold_in(splits[3], 1), 0, LEVELS - 1).astype(jnp.int32),
        "visible": plant((jax.random.randint(splits[4], (GROUPS, GROUPS), 0, 3) < 2).astype(jnp.int32), jax.random.fold_in(splits[4], 1), 0, 1),
        "level_gates": jnp.clip(jax.random.uniform(splits[5], (LEVELS, WIDTH), jnp.float32, 0.5, 2.0), 0.5, 2.0),
    }


NEGATIVE = -1e+30

def reference(queries, key_vectors, value_vectors, noise_levels, visible, level_gates):
    group_tok = TOKENS // GROUPS
    score_scale = 1.0 / math.sqrt(HEAD_DIM)
    query_heads = queries.reshape(TOKENS, HEADS, HEAD_DIM).transpose(1, 0, 2)
    key_heads = key_vectors.reshape(TOKENS, HEADS, HEAD_DIM).transpose(1, 0, 2)
    value_heads = value_vectors.reshape(TOKENS, HEADS, HEAD_DIM).transpose(1, 0, 2)
    results = []
    for group in range(GROUPS):
        limit = (group + 1) * group_tok
        key_group = (jnp.arange(limit, dtype=jnp.int32) // group_tok).astype(jnp.int32)
        row_flags = visible[group][key_group]
        live = (key_group == group) | (key_group < group) & (row_flags == 1)

        def one_head(operands):
            query_part, key_part, value_part = operands
            score = jnp.dot(query_part, key_part.T, preferred_element_type=jnp.float32) * score_scale
            score = jnp.where(live[None, :], score, NEGATIVE)
            rowmax = lax.optimization_barrier(jnp.max(score, axis=1, keepdims=True))
            weight = jnp.where(live[None, :], jnp.exp(score - rowmax), 0.0)
            denominator = lax.optimization_barrier(jnp.sum(weight, axis=1, keepdims=True))
            numerator = jnp.dot(weight.astype(jnp.bfloat16), value_part, preferred_element_type=jnp.float32)
            return numerator / denominator
        heads_out = lax.map(one_head, (query_heads[:, group * group_tok:limit], key_heads[:, :limit], value_heads[:, :limit]))
        gate_row = level_gates[noise_levels[group]]
        joined = heads_out.transpose(1, 0, 2).reshape(group_tok, WIDTH) * gate_row[None, :]
        results.append(joined.astype(jnp.bfloat16))
    return jnp.concatenate(results, axis=0)
```

```python
import functools
import math

import jax
import jax.numpy as jnp
from jax import lax
from jax.experimental import pallas as pl
from jax.experimental.pallas import tpu as pltpu
from jax.sharding import Mesh
from jax.sharding import PartitionSpec as P

HEAD_DIM = 128
AXES = ("z", "yh", "yl", "x", "core")
HEAD_AXES = ("z", "yh", "yl")
NEGATIVE = -1e30
TO_EXP2 = math.log2(math.e) / math.sqrt(HEAD_DIM)


def attend(pieces, slots, pair_query, pair_key, pair_slot, steps, noise, q_ref, *refs):
    k_refs = refs[:pieces]
    v_refs = refs[pieces : 2 * pieces]
    gate_ref, o_ref, score_a, score_b, m_ref, l_ref, acc_ref = refs[2 * pieces :]
    m_ref[...] = jnp.full_like(m_ref, NEGATIVE)
    l_ref[...] = jnp.zeros_like(l_ref)
    acc_ref[...] = jnp.zeros_like(acc_ref)

    def scores(i, score_ref):
        keys = jnp.concatenate([k[pair_key[i]] for k in k_refs], axis=0)
        score_ref[...] = lax.dot_general(
            q_ref[pair_query[i]], keys, (((1,), (1,)), ((), ())), preferred_element_type=jnp.float32
        )

    def fold(i, score_ref):
        slot = pair_slot[i]
        values = jnp.concatenate([v[pair_key[i]] for v in v_refs], axis=0)
        score = score_ref[...]
        old = m_ref[slot]
        new = jnp.maximum(old, jnp.max(score, axis=1, keepdims=True))
        weight = jnp.exp2((score - new) * TO_EXP2)
        factor = jnp.exp2((old - new) * TO_EXP2)
        m_ref[slot] = new
        l_ref[slot] = l_ref[slot] * factor + jnp.sum(weight, axis=1, keepdims=True)
        acc_ref[slot] = acc_ref[slot] * factor + jnp.dot(
            weight.astype(jnp.bfloat16), values, preferred_element_type=jnp.float32
        )

    scores(0, score_a)

    def step(j, carry):
        scores(2 * j + 1, score_b)
        fold(2 * j, score_a)
        scores(2 * j + 2, score_a)
        fold(2 * j + 1, score_b)
        return carry

    lax.fori_loop(0, steps[0], step, 0)

    def finish(c, carry):
        gate = gate_ref[pl.ds(noise[c], 1), :]
        o_ref[c] = (acc_ref[c] / l_ref[c] * gate).astype(o_ref.dtype)
        return carry

    lax.fori_loop(0, slots, finish, 0)


def live_pairs(visible):
    groups = visible.shape[0]
    total = groups * groups
    length = groups * (groups + 1) // 2 + 3
    ids = jnp.arange(total, dtype=jnp.int32)
    c, e = ids // groups, ids % groups
    live = (c == e) | (e < c) & (visible.reshape(-1) == 1)
    place = jnp.sum((live[None, :] & (ids[None, :] < ids[:, None])).astype(jnp.int32), axis=1)
    taken = live[None, :] & (place[None, :] == jnp.arange(length, dtype=jnp.int32)[:, None])
    found = jnp.any(taken, axis=1)
    pair = jnp.sum(jnp.where(taken, ids[None, :], 0), axis=1)
    count = jnp.sum(live.astype(jnp.int32))
    query = pair // groups
    return query, pair % groups, jnp.where(found, query, groups), ((count + 1) // 2).reshape(1)


def on_device(queries, key_vectors, value_vectors, noise_levels, visible, level_gates):
    peers = lax.axis_size(HEAD_AXES)
    groups = visible.shape[0]
    heads = queries.shape[1] // HEAD_DIM

    def to_heads(value):
        blocks = value.reshape(value.shape[0], heads, HEAD_DIM).transpose(1, 0, 2)
        return lax.all_to_all(blocks, HEAD_AXES, 0, 0, tiled=True).reshape(groups, -1, HEAD_DIM)

    def swapped(value):
        return lax.ppermute(value, "core", [(0, 1), (1, 0)])

    def gathered(value):
        size = lax.axis_size("x")
        pieces = [value]
        for shift in (1, size - 1, 2):
            pieces.append(lax.ppermute(value, "x", [(i, (i + shift) % size) for i in range(size)]))
        return pieces + [swapped(piece) for piece in pieces]

    keys = gathered(to_heads(key_vectors))
    values = gathered(to_heads(value_vectors))
    query = to_heads(queries)
    rows = query.shape[1]
    pair_query, pair_key, pair_slot, steps = live_pairs(visible)
    head = lax.axis_index(HEAD_AXES)
    gates = lax.dynamic_slice_in_dim(level_gates, head * HEAD_DIM, HEAD_DIM, axis=1)
    pieces = len(keys)
    width = pieces * rows
    vmem = pl.BlockSpec(memory_space=pltpu.VMEM)
    smem = pl.BlockSpec(memory_space=pltpu.SMEM)
    blocks = groups * (groups + 1) // 2
    out = pl.pallas_call(
        functools.partial(attend, pieces, groups),
        out_shape=jax.ShapeDtypeStruct(query.shape, jnp.bfloat16),
        in_specs=[smem] * 5 + [vmem] * (2 + 2 * pieces),
        out_specs=vmem,
        scratch_shapes=[
            pltpu.VMEM((rows, width), jnp.float32),
            pltpu.VMEM((rows, width), jnp.float32),
            pltpu.VMEM((groups + 1, rows, 1), jnp.float32),
            pltpu.VMEM((groups + 1, rows, 1), jnp.float32),
            pltpu.VMEM((groups + 1, rows, HEAD_DIM), jnp.float32),
        ],
        compiler_params=pltpu.CompilerParams(vmem_limit_bytes=40 * 1024 * 1024),
        cost_estimate=pl.CostEstimate(
            flops=4 * blocks * rows * width * HEAD_DIM,
            bytes_accessed=4 * pieces * query.size,
            transcendentals=blocks * rows * width,
        ),
        name="attend",
    )(pair_query, pair_key, pair_slot, steps, noise_levels, query, *keys, *values, gates)
    back = out.reshape(peers, -1, HEAD_DIM)
    back = lax.all_to_all(back, HEAD_AXES, 0, 0, tiled=True)
    return back.transpose(1, 0, 2).reshape(queries.shape)


def solution(mesh):
    split = Mesh(mesh.devices.reshape(8, 2, 2, 4, 2), AXES)
    rows = P(AXES, None)
    return jax.shard_map(
        on_device,
        mesh=split,
        in_specs=(rows, rows, rows, P(), P(), P()),
        out_specs=rows,
        check_vma=False,
    )
```

```python
import functools
import math

import jax
import jax.numpy as jnp
from jax import lax
from jax.experimental import pallas as pl
from jax.experimental.pallas import tpu as pltpu
from jax.sharding import Mesh
from jax.sharding import PartitionSpec as P

HEAD_DIM = 128
AXES = ("z", "yh", "yl", "x", "core")
HEAD_AXES = ("z", "yh", "yl")
NEGATIVE = -1e30
UNROLL = 4
TO_EXP2 = math.log2(math.e) / math.sqrt(HEAD_DIM)


def attend(sources, first, last, groups, lists, noise, q_ref, *refs):
    refs = list(refs)
    keys, values = [], []
    for kind in sources:
        if kind == "pair":
            ref = refs.pop(0)
            keys.append(ref.at[0])
            values.append(ref.at[1])
        else:
            keys.append(refs.pop(0))
            values.append(refs.pop(0))
    if not first:
        old_m, old_l, old_acc = refs[:3]
        refs = refs[3:]
    if last:
        gate_ref, o_ref, m_ref, l_ref, acc_ref, turned_ref, padded_ref, *scores_ref = refs
    else:
        m_ref, l_ref, acc_ref, turned_ref, padded_ref, *scores_ref = refs
    if first:
        m_ref[...] = jnp.full_like(m_ref, NEGATIVE)
        l_ref[...] = jnp.zeros_like(l_ref)
        acc_ref[...] = jnp.zeros_like(acc_ref)
    else:
        m_ref[...] = old_m[...]
        l_ref[...] = old_l[...]
        acc_ref[...] = old_acc[...]

    pad = HEAD_DIM - q_ref.shape[1]

    def prepare(c, carry):
        turned_ref[c] = jnp.concatenate([v[c] for v in values], axis=0).T
        padded_ref[c] = jnp.concatenate([q_ref[c], jnp.zeros((pad, HEAD_DIM), q_ref.dtype)], axis=0)
        return carry

    lax.fori_loop(0, groups, prepare, 0, unroll=4)

    def scores(i, score_ref):
        block = jnp.concatenate([k[lists[2, i]] for k in keys], axis=0)
        query = jnp.concatenate([padded_ref[lists[0, i]], padded_ref[lists[1, i]]], axis=0)
        score_ref[...] = lax.dot_general(
            block, query, (((1,), (1,)), ((), ())), preferred_element_type=jnp.float32
        )

    def weigh(i, u):
        score = scores_ref[u]
        high = jnp.max(score[...], axis=0, keepdims=True)
        weight = jnp.exp2((score[...] - high) * TO_EXP2)
        total = jnp.sum(weight, axis=0, keepdims=True)
        update = jnp.dot(
            turned_ref[lists[2, i]], weight.astype(jnp.bfloat16), preferred_element_type=jnp.float32
        )
        return high, total, update

    def merge(i, found):
        high, total, update = found
        for part in range(2):
            slot = lists[3 + part, i]
            lanes = slice(part * HEAD_DIM, (part + 1) * HEAD_DIM)
            old = m_ref[slot]
            new = jnp.maximum(old, high[:, lanes])
            keep = jnp.exp2((old - new) * TO_EXP2)
            take = jnp.exp2((high[:, lanes] - new) * TO_EXP2)
            m_ref[slot] = new
            l_ref[slot] = l_ref[slot] * keep + total[:, lanes] * take
            acc_ref[slot] = acc_ref[slot] * keep + update[:, lanes] * take

    for u in range(UNROLL):
        scores(u, scores_ref[u])

    def step(j, carry):
        found = []
        for u in range(UNROLL):
            found.append(weigh(UNROLL * j + u, u))
            scores(UNROLL * (j + 1) + u, scores_ref[u])
        for u in range(UNROLL):
            merge(UNROLL * j + u, found[u])
        return carry

    lax.fori_loop(0, lists[5, 0], step, 0)

    if last:

        def finish(c, carry):
            gate = gate_ref[pl.ds(noise[c], 1), :]
            ratio = (acc_ref[c] / l_ref[c]).T[: q_ref.shape[1]]
            o_ref[c] = (ratio * gate).astype(o_ref.dtype)
            return carry

        lax.fori_loop(0, groups, finish, 0, unroll=4)


def attend_call(sources, first, last, lists, noise, query, operands):
    groups, rows, _ = query.shape
    width = len(sources) * rows
    blocks = groups * (groups + 1) // 2
    vmem = pl.BlockSpec(memory_space=pltpu.VMEM)
    smem = pl.BlockSpec(memory_space=pltpu.SMEM)
    state = [(groups + 1, 1, HEAD_DIM), (groups + 1, 1, HEAD_DIM), (groups + 1, HEAD_DIM, HEAD_DIM)]
    work = [
        pltpu.VMEM((groups, HEAD_DIM, width), jnp.bfloat16),
        pltpu.VMEM((groups, HEAD_DIM, HEAD_DIM), jnp.bfloat16),
    ] + [pltpu.VMEM((width, 2 * HEAD_DIM), jnp.float32)] * UNROLL
    if last:
        out_shape = jax.ShapeDtypeStruct(query.shape, jnp.bfloat16)
        scratch = [pltpu.VMEM(shape, jnp.float32) for shape in state] + work
    else:
        out_shape = [jax.ShapeDtypeStruct(shape, jnp.float32) for shape in state]
        scratch = work
    return pl.pallas_call(
        functools.partial(attend, sources, first, last, groups),
        out_shape=out_shape,
        in_specs=[smem, smem] + [vmem] * (1 + len(operands)),
        out_specs=vmem if last else [vmem] * 3,
        scratch_shapes=scratch,
        compiler_params=pltpu.CompilerParams(vmem_limit_bytes=16 * 1024 * 1024),
        cost_estimate=pl.CostEstimate(
            flops=12 * blocks * rows * width * HEAD_DIM,
            bytes_accessed=4 * len(sources) * query.size,
            transcendentals=blocks * rows * width,
        ),
        name="attend_last" if last else "attend_first",
    )(lists, noise, query, *operands)


def live_pairs(visible):
    groups = visible.shape[0]
    ids = jnp.arange(groups, dtype=jnp.int32)
    c, e = ids[:, None], ids[None, :]
    live = (c == e) | (e < c) & (visible == 1)
    rank = jnp.sum((live[None, :, :] & (ids[None, :] < ids[:, None])[:, :, None]).astype(jnp.int32), axis=1)
    seen = jnp.sum(live.astype(jnp.int32), axis=0)
    pairs = (seen + 1) // 2
    start = jnp.sum(jnp.where(ids[None, :] < ids[:, None], pairs[None, :], 0), axis=1)
    total = jnp.sum(pairs)
    length = sum((n + 1) // 2 for n in range(1, groups + 1)) + 2 * UNROLL - 1
    places = jnp.arange(length, dtype=jnp.int32)
    column = start[None, :] + rank // 2
    rows = []
    for part in range(2):
        here = live & (rank % 2 == part)
        taken = here[None, :, :] & (column[None, :, :] == places[:, None, None])
        found = jnp.any(taken, axis=(1, 2))
        query = jnp.sum(jnp.where(taken, ids[None, :, None], 0), axis=(1, 2))
        key = jnp.sum(jnp.where(taken, ids[None, None, :], 0), axis=(1, 2))
        rows.append((query, key, jnp.where(found, query, groups)))
    (q0, key, s0), (q1, _, s1) = rows
    steps = jnp.broadcast_to((total + UNROLL - 1) // UNROLL, places.shape)
    return jnp.stack([q0, q1, key, s0, s1, steps])


def to_heads(value):
    return value.reshape(value.shape[0], -1, HEAD_DIM).transpose(1, 0, 2)


def pack(k_ref, v_ref, o_ref):
    for h in range(o_ref.shape[0]):
        lanes = slice(h * HEAD_DIM, (h + 1) * HEAD_DIM)
        o_ref[h, 0] = k_ref[:, lanes]
        o_ref[h, 1] = v_ref[:, lanes]


def packed(keys, values):
    tokens, width = keys.shape
    vmem = pl.BlockSpec(memory_space=pltpu.VMEM)
    return pl.pallas_call(
        pack,
        out_shape=jax.ShapeDtypeStruct((width // HEAD_DIM, 2, tokens, HEAD_DIM), keys.dtype),
        in_specs=[vmem, vmem],
        out_specs=vmem,
        compiler_params=pltpu.CompilerParams(vmem_limit_bytes=8 * 1024 * 1024),
        name="pack",
    )(keys, values)


def swapped(value):
    return lax.ppermute(value, "core", [(0, 1), (1, 0)])


def shifted(value, shift):
    size = lax.axis_size("x")
    return lax.ppermute(value, "x", [(i, (i + shift) % size) for i in range(size)])


def on_device(queries, key_vectors, value_vectors, noise_levels, visible, level_gates):
    groups = visible.shape[0]
    tokens = queries.shape[0]
    pair = lax.all_to_all(packed(key_vectors, value_vectors), HEAD_AXES, 0, 0, tiled=True)
    pair = pair.reshape(groups, -1, 2, tokens, HEAD_DIM).transpose(2, 0, 1, 3, 4)
    pair = pair.reshape(2, groups, -1, HEAD_DIM)
    query = lax.all_to_all(to_heads(queries), HEAD_AXES, 0, 0, tiled=True).reshape(groups, -1, HEAD_DIM)
    above, below = shifted(pair, 1), shifted(pair, -1)
    far = [shifted(above[0], 1), shifted(below[1], -1)]
    lists = live_pairs(visible)
    head = lax.axis_index(HEAD_AXES)
    gates = lax.dynamic_slice_in_dim(level_gates, head * HEAD_DIM, HEAD_DIM, axis=1)
    early = [pair, above, swapped(pair), swapped(above)]
    late = [below, swapped(below)]
    state = attend_call(["pair"] * 4, True, False, lists, noise_levels, query, early)
    far, state = lax.optimization_barrier((far, state))
    late = late + far + [swapped(piece) for piece in far] + list(state) + [gates]
    out = attend_call(["pair"] * 2 + ["two"] * 2, False, True, lists, noise_levels, query, late)
    back = out.reshape(lax.axis_size(HEAD_AXES), -1, HEAD_DIM)
    back = lax.all_to_all(back, HEAD_AXES, 0, 0, tiled=True)
    return back.transpose(1, 0, 2).reshape(queries.shape)


def solution(mesh):
    split = Mesh(mesh.devices.reshape(8, 2, 2, 4, 2), AXES)
    rows = P(AXES, None)
    return jax.shard_map(
        on_device,
        mesh=split,
        in_specs=(rows, rows, rows, P(), P(), P()),
        out_specs=rows,
        check_vma=False,
    )
```

```python
import functools
import math

import jax
import jax.numpy as jnp
from jax import lax
from jax.experimental import pallas as pl
from jax.experimental.pallas import tpu as pltpu
from jax.sharding import Mesh
from jax.sharding import PartitionSpec as P


HEAD_DIM = 128
AXES = ("z", "yh", "yl", "x", "core")
HEAD_AXES = ("z", "yh", "yl")
NEGATIVE = -1e30
UNROLL = 4
TO_EXP2 = math.log2(math.e) / math.sqrt(HEAD_DIM)


def attend(sources, first, last, groups, lists, noise, q_ref, *refs):
    refs = list(refs)
    keys, values = [], []
    for kind in sources:
        if kind == "pair":
            ref = refs.pop(0)
            keys.append(ref.at[0])
            values.append(ref.at[1])
        else:
            keys.append(refs.pop(0))
            values.append(refs.pop(0))
    if not first:
        old_m, old_l, old_acc = refs[:3]
        refs = refs[3:]
    if last:
        gate_ref, o_ref, m_ref, l_ref, acc_ref, turned_ref, padded_ref, *scores_ref, done = refs
    else:
        m_ref, l_ref, acc_out, acc_ref, turned_ref, padded_ref, *scores_ref, done = refs
    if first:
        m_ref[...] = jnp.full_like(m_ref, NEGATIVE)
        l_ref[...] = jnp.zeros_like(l_ref)
        acc_ref[...] = jnp.zeros_like(acc_ref)
    else:
        m_ref[...] = old_m[...]
        l_ref[...] = old_l[...]
        fetch = pltpu.make_async_copy(old_acc, acc_ref, done)
        fetch.start()

    pad = HEAD_DIM - q_ref.shape[1]

    def prepare(c, carry):
        turned_ref[c] = jnp.concatenate([v[c] for v in values], axis=0).T
        padded_ref[c] = jnp.concatenate([q_ref[c], jnp.zeros((pad, HEAD_DIM), q_ref.dtype)], axis=0)
        return carry

    lax.fori_loop(0, groups, prepare, 0, unroll=4)

    def scores(i, score_ref):
        block = jnp.concatenate([k[lists[2, i]] for k in keys], axis=0)
        query = jnp.concatenate([padded_ref[lists[0, i]], padded_ref[lists[1, i]]], axis=0)
        score_ref[...] = lax.dot_general(
            block, query, (((1,), (1,)), ((), ())), preferred_element_type=jnp.float32
        )

    def weigh(i, u):
        score = scores_ref[u]
        high = jnp.max(score[...], axis=0, keepdims=True)
        weight = jnp.exp2((score[...] - high) * TO_EXP2)
        total = jnp.sum(weight, axis=0, keepdims=True)
        update = jnp.dot(
            turned_ref[lists[2, i]], weight.astype(jnp.bfloat16), preferred_element_type=jnp.float32
        )
        return high, total, update

    def merge(i, found):
        high, total, update = found
        for part in range(2):
            slot = lists[3 + part, i]
            lanes = slice(part * HEAD_DIM, (part + 1) * HEAD_DIM)
            old = m_ref[slot]
            new = jnp.maximum(old, high[:, lanes])
            keep = jnp.exp2((old - new) * TO_EXP2)
            take = jnp.exp2((high[:, lanes] - new) * TO_EXP2)
            m_ref[slot] = new
            l_ref[slot] = l_ref[slot] * keep + total[:, lanes] * take
            acc_ref[slot] = acc_ref[slot] * keep + update[:, lanes] * take

    for u in range(UNROLL):
        scores(u, scores_ref[u])

    def step(j, carry):
        found = []
        for u in range(UNROLL):
            found.append(weigh(UNROLL * j + u, u))
            scores(UNROLL * (j + 1) + u, scores_ref[u])
        for u in range(UNROLL):
            merge(UNROLL * j + u, found[u])
        return carry

    if not first:
        fetch.wait()

    lax.fori_loop(0, lists[5, 0], step, 0)

    if not last:
        store = pltpu.make_async_copy(acc_ref, acc_out, done)
        store.start()
        store.wait()

    if last:

        def finish(c, carry):
            gate = gate_ref[pl.ds(noise[c], 1), :]
            ratio = (acc_ref[c] / l_ref[c]).T[: q_ref.shape[1]]
            o_ref[c] = (ratio * gate).astype(o_ref.dtype)
            return carry

        lax.fori_loop(0, groups, finish, 0, unroll=4)


def attend_call(sources, first, last, lists, noise, query, operands):
    groups, rows, _ = query.shape
    width = len(sources) * rows
    blocks = groups * (groups + 1) // 2
    vmem = pl.BlockSpec(memory_space=pltpu.VMEM)
    smem = pl.BlockSpec(memory_space=pltpu.SMEM)
    state = [(groups + 1, 1, HEAD_DIM), (groups + 1, 1, HEAD_DIM), (groups + 1, HEAD_DIM, HEAD_DIM)]
    work = [
        pltpu.VMEM((groups, HEAD_DIM, width), jnp.bfloat16),
        pltpu.VMEM((groups, HEAD_DIM, HEAD_DIM), jnp.bfloat16),
    ] + [pltpu.VMEM((width, 2 * HEAD_DIM), jnp.float32)] * UNROLL
    if last:
        out_shape = jax.ShapeDtypeStruct(query.shape, jnp.bfloat16)
        scratch = [pltpu.VMEM(shape, jnp.float32) for shape in state] + work
        out_specs = vmem
    else:
        out_shape = [jax.ShapeDtypeStruct(shape, jnp.float32) for shape in state]
        scratch = [pltpu.VMEM(state[2], jnp.float32)] + work
        out_specs = [vmem, vmem, pl.BlockSpec(memory_space=pltpu.HBM)]
    in_specs = [smem, smem] + [vmem] * (1 + len(operands))
    if not first:
        in_specs[-2 if last else -1] = pl.BlockSpec(memory_space=pltpu.HBM)
    return pl.pallas_call(
        functools.partial(attend, sources, first, last, groups),
        out_shape=out_shape,
        in_specs=in_specs,
        out_specs=out_specs,
        scratch_shapes=scratch + [pltpu.SemaphoreType.DMA],
        compiler_params=pltpu.CompilerParams(vmem_limit_bytes=16 * 1024 * 1024),
        cost_estimate=pl.CostEstimate(
            flops=12 * blocks * rows * width * HEAD_DIM,
            bytes_accessed=4 * len(sources) * query.size,
            transcendentals=blocks * rows * width,
        ),
        name="attend_last" if last else "attend_first",
    )(lists, noise, query, *operands)


def live_pairs(visible):
    groups = visible.shape[0]
    ids = jnp.arange(groups, dtype=jnp.int32)
    c, e = ids[:, None], ids[None, :]
    live = (c == e) | (e < c) & (visible == 1)
    rank = jnp.sum((live[None, :, :] & (ids[None, :] < ids[:, None])[:, :, None]).astype(jnp.int32), axis=1)
    seen = jnp.sum(live.astype(jnp.int32), axis=0)
    pairs = (seen + 1) // 2
    start = jnp.sum(jnp.where(ids[None, :] < ids[:, None], pairs[None, :], 0), axis=1)
    total = jnp.sum(pairs)
    length = sum((n + 1) // 2 for n in range(1, groups + 1)) + 2 * UNROLL - 1
    places = jnp.arange(length, dtype=jnp.int32)
    column = start[None, :] + rank // 2
    rows = []
    for part in range(2):
        here = live & (rank % 2 == part)
        taken = here[None, :, :] & (column[None, :, :] == places[:, None, None])
        found = jnp.any(taken, axis=(1, 2))
        query = jnp.sum(jnp.where(taken, ids[None, :, None], 0), axis=(1, 2))
        key = jnp.sum(jnp.where(taken, ids[None, None, :], 0), axis=(1, 2))
        rows.append((query, key, jnp.where(found, query, groups)))
    (q0, key, s0), (q1, _, s1) = rows
    steps = jnp.broadcast_to((total + UNROLL - 1) // UNROLL, places.shape)
    return jnp.stack([q0, q1, key, s0, s1, steps])


def to_heads(value):
    return value.reshape(value.shape[0], -1, HEAD_DIM).transpose(1, 0, 2)


def pack(k_ref, v_ref, o_ref):
    for h in range(o_ref.shape[0]):
        lanes = slice(h * HEAD_DIM, (h + 1) * HEAD_DIM)
        o_ref[h, 0] = k_ref[:, lanes]
        o_ref[h, 1] = v_ref[:, lanes]


def packed(keys, values):
    tokens, width = keys.shape
    vmem = pl.BlockSpec(memory_space=pltpu.VMEM)
    return pl.pallas_call(
        pack,
        out_shape=jax.ShapeDtypeStruct((width // HEAD_DIM, 2, tokens, HEAD_DIM), keys.dtype),
        in_specs=[vmem, vmem],
        out_specs=vmem,
        compiler_params=pltpu.CompilerParams(vmem_limit_bytes=8 * 1024 * 1024),
        name="pack",
    )(keys, values)


def swapped(value):
    return lax.ppermute(value, "core", [(0, 1), (1, 0)])


def shifted(value, shift):
    size = lax.axis_size("x")
    return lax.ppermute(value, "x", [(i, (i + shift) % size) for i in range(size)])


def exchanged(blocks):
    return lax.all_to_all(blocks, HEAD_AXES, 0, 0, tiled=True)


def attention(queries, key_vectors, value_vectors, noise_levels, visible, level_gates):
    groups = visible.shape[0]
    pair = exchanged(packed(key_vectors, value_vectors))
    key = pair[:, 0].reshape(groups, -1, HEAD_DIM)
    value = pair[:, 1].reshape(groups, -1, HEAD_DIM)
    query = exchanged(to_heads(queries)).reshape(groups, -1, HEAD_DIM)
    key_up, key_down = shifted(key, 1), shifted(key, -1)
    value_up, value_down = shifted(value, 1), shifted(value, -1)
    key_far, value_far = shifted(key_up, 1), shifted(value_down, -1)
    lists = live_pairs(visible)
    head = lax.axis_index(HEAD_AXES)
    gates = lax.dynamic_slice_in_dim(level_gates, head * HEAD_DIM, HEAD_DIM, axis=1)
    early = [key, value, key_up, value_up]
    early = early + [swapped(piece) for piece in early]
    late = [key_down, value_down]
    late = late + [swapped(piece) for piece in late]
    state = attend_call(["two"] * 4, True, False, lists, noise_levels, query, early)
    key_far, value_far, top = lax.optimization_barrier((key_far, value_far, state[0]))
    late = late + [key_far, value_far, swapped(key_far), swapped(value_far), top, *state[1:], gates]
    out = attend_call(["two"] * 4, False, True, lists, noise_levels, query, late)
    back = out.reshape(lax.axis_size(HEAD_AXES), -1, HEAD_DIM)
    back = lax.all_to_all(back, HEAD_AXES, 0, 0, tiled=True)
    return back.transpose(1, 0, 2).reshape(queries.shape)


def solution(mesh):
    split = Mesh(mesh.devices.reshape(8, 2, 2, 4, 2), AXES)
    rows = P(AXES, None)
    return jax.shard_map(
        attention,
        mesh=split,
        in_specs=(rows, rows, rows, P(), P(), P()),
        out_specs=rows,
        check_vma=False,
    )
```

```python
import functools
import math

import jax
import jax.numpy as jnp
from jax import lax
from jax.experimental import pallas as pl
from jax.experimental.pallas import tpu as pltpu
from jax.sharding import Mesh
from jax.sharding import PartitionSpec as P


HEAD_DIM = 128
AXES = ("z", "yh", "yl", "x", "core")
HEAD_AXES = ("z", "yh", "yl")
NEGATIVE = -1e30
UNROLL = 4
TO_EXP2 = math.log2(math.e) / math.sqrt(HEAD_DIM)


def attend(sources, first, last, groups, lists, noise, q_ref, *refs):
    refs = list(refs)
    keys, values = [], []
    for kind in sources:
        if kind == "pair":
            ref = refs.pop(0)
            keys.append(ref.at[0])
            values.append(ref.at[1])
        else:
            keys.append(refs.pop(0))
            values.append(refs.pop(0))
    if not first:
        old_m, old_l, old_acc = refs[:3]
        refs = refs[3:]
    if last:
        gate_ref, o_ref, m_ref, l_ref, acc_ref, turned_ref, padded_ref, *scores_ref, done = refs
    else:
        m_ref, l_ref, acc_out, acc_ref, turned_ref, padded_ref, *scores_ref, done = refs
    if first:
        m_ref[...] = jnp.full_like(m_ref, NEGATIVE)
        l_ref[...] = jnp.zeros_like(l_ref)
        acc_ref[...] = jnp.zeros_like(acc_ref)
    else:
        m_ref[...] = old_m[...]
        l_ref[...] = old_l[...]
        fetch = pltpu.make_async_copy(old_acc.at[: groups + 1], acc_ref, done)
        fetch.start()

    pad = HEAD_DIM - q_ref.shape[1]

    def prepare(c, carry):
        turned_ref[c] = jnp.concatenate([v[c] for v in values], axis=0).T
        padded_ref[c] = jnp.concatenate([q_ref[c], jnp.zeros((pad, HEAD_DIM), q_ref.dtype)], axis=0)
        return carry

    lax.fori_loop(0, groups, prepare, 0, unroll=4)

    def scores(i, score_ref):
        block = jnp.concatenate([k[lists[2, i]] for k in keys], axis=0)
        query = jnp.concatenate([padded_ref[lists[0, i]], padded_ref[lists[1, i]]], axis=0)
        score_ref[...] = lax.dot_general(
            block, query, (((1,), (1,)), ((), ())), preferred_element_type=jnp.float32
        )

    def weigh(i, u):
        score = scores_ref[u]
        high = jnp.max(score[...], axis=0, keepdims=True)
        weight = jnp.exp2((score[...] - high) * TO_EXP2)
        total = jnp.sum(weight, axis=0, keepdims=True)
        update = jnp.dot(
            turned_ref[lists[2, i]], weight.astype(jnp.bfloat16), preferred_element_type=jnp.float32
        )
        return high, total, update

    def merge(i, found):
        high, total, update = found
        for part in range(2):
            slot = lists[3 + part, i]
            lanes = slice(part * HEAD_DIM, (part + 1) * HEAD_DIM)
            old = m_ref[slot]
            new = jnp.maximum(old, high[:, lanes])
            keep = jnp.exp2((old - new) * TO_EXP2)
            take = jnp.exp2((high[:, lanes] - new) * TO_EXP2)
            m_ref[slot] = new
            l_ref[slot] = l_ref[slot] * keep + total[:, lanes] * take
            acc_ref[slot] = acc_ref[slot] * keep + update[:, lanes] * take

    for u in range(UNROLL):
        scores(u, scores_ref[u])

    def step(j, carry):
        found = []
        for u in range(UNROLL):
            found.append(weigh(UNROLL * j + u, u))
            scores(UNROLL * (j + 1) + u, scores_ref[u])
        for u in range(UNROLL):
            merge(UNROLL * j + u, found[u])
        return carry

    if not first:
        fetch.wait()

    lax.fori_loop(0, lists[5, 0], step, 0)

    if not last:
        store = pltpu.make_async_copy(acc_ref, acc_out.at[: groups + 1], done)
        store.start()
        store.wait()

    if last:

        def finish(c, carry):
            gate = gate_ref[pl.ds(noise[c], 1), :]
            ratio = (acc_ref[c] / l_ref[c]).T[: q_ref.shape[1]]
            o_ref[c] = (ratio * gate).astype(o_ref.dtype)
            return carry

        lax.fori_loop(0, groups, finish, 0, unroll=4)


def attend_call(sources, first, last, lists, noise, query, operands):
    groups, rows, _ = query.shape
    width = len(sources) * rows
    blocks = groups * (groups + 1) // 2
    vmem = pl.BlockSpec(memory_space=pltpu.VMEM)
    smem = pl.BlockSpec(memory_space=pltpu.SMEM)
    state = [(groups + 1, 1, HEAD_DIM), (groups + 1, 1, HEAD_DIM), (groups + 1, HEAD_DIM, HEAD_DIM)]
    work = [
        pltpu.VMEM((groups, HEAD_DIM, width), jnp.bfloat16),
        pltpu.VMEM((groups, HEAD_DIM, HEAD_DIM), jnp.bfloat16),
    ] + [pltpu.VMEM((width, 2 * HEAD_DIM), jnp.float32)] * UNROLL
    if last:
        out_shape = jax.ShapeDtypeStruct(query.shape, jnp.bfloat16)
        scratch = [pltpu.VMEM(shape, jnp.float32) for shape in state] + work
        out_specs = vmem
    else:
        roomy = (8 * (groups + 1), *state[2][1:])
        out_shape = [jax.ShapeDtypeStruct(shape, jnp.float32) for shape in (*state[:2], roomy)]
        scratch = [pltpu.VMEM(state[2], jnp.float32)] + work
        out_specs = [vmem, vmem, pl.BlockSpec(memory_space=pltpu.HBM)]
    in_specs = [smem, smem] + [vmem] * (1 + len(operands))
    if not first:
        in_specs[-2 if last else -1] = pl.BlockSpec(memory_space=pltpu.HBM)
    return pl.pallas_call(
        functools.partial(attend, sources, first, last, groups),
        out_shape=out_shape,
        in_specs=in_specs,
        out_specs=out_specs,
        scratch_shapes=scratch + [pltpu.SemaphoreType.DMA],
        compiler_params=pltpu.CompilerParams(vmem_limit_bytes=16 * 1024 * 1024),
        cost_estimate=pl.CostEstimate(
            flops=12 * blocks * rows * width * HEAD_DIM,
            bytes_accessed=4 * len(sources) * query.size,
            transcendentals=blocks * rows * width,
        ),
        name="attend_last" if last else "attend_first",
    )(lists, noise, query, *operands)


def live_pairs(visible):
    groups = visible.shape[0]
    ids = jnp.arange(groups, dtype=jnp.int32)
    c, e = ids[:, None], ids[None, :]
    live = (c == e) | (e < c) & (visible == 1)
    rank = jnp.sum((live[None, :, :] & (ids[None, :] < ids[:, None])[:, :, None]).astype(jnp.int32), axis=1)
    seen = jnp.sum(live.astype(jnp.int32), axis=0)
    pairs = (seen + 1) // 2
    start = jnp.sum(jnp.where(ids[None, :] < ids[:, None], pairs[None, :], 0), axis=1)
    total = jnp.sum(pairs)
    length = sum((n + 1) // 2 for n in range(1, groups + 1)) + 2 * UNROLL - 1
    places = jnp.arange(length, dtype=jnp.int32)
    column = start[None, :] + rank // 2
    rows = []
    for part in range(2):
        here = live & (rank % 2 == part)
        taken = here[None, :, :] & (column[None, :, :] == places[:, None, None])
        found = jnp.any(taken, axis=(1, 2))
        query = jnp.sum(jnp.where(taken, ids[None, :, None], 0), axis=(1, 2))
        key = jnp.sum(jnp.where(taken, ids[None, None, :], 0), axis=(1, 2))
        rows.append((query, key, jnp.where(found, query, groups)))
    (q0, key, s0), (q1, _, s1) = rows
    steps = jnp.broadcast_to((total + UNROLL - 1) // UNROLL, places.shape)
    return jnp.stack([q0, q1, key, s0, s1, steps])


def to_heads(value):
    return value.reshape(value.shape[0], -1, HEAD_DIM).transpose(1, 0, 2)


def pack(k_hbm, v_hbm, o_ref, k_ref, v_ref, done):
    fetches = [pltpu.make_async_copy(k_hbm, k_ref, done.at[0]), pltpu.make_async_copy(v_hbm, v_ref, done.at[1])]
    for fetch in fetches:
        fetch.start()
    for i, ref in enumerate((k_ref, v_ref)):
        fetches[i].wait()
        for h in range(o_ref.shape[0]):
            o_ref[h, i] = ref[:, h * HEAD_DIM : (h + 1) * HEAD_DIM]


def packed(keys, values):
    tokens, width = keys.shape
    hbm = pl.BlockSpec(memory_space=pltpu.HBM)
    return pl.pallas_call(
        pack,
        out_shape=jax.ShapeDtypeStruct((width // HEAD_DIM, 2, tokens, HEAD_DIM), keys.dtype),
        in_specs=[hbm, hbm],
        out_specs=pl.BlockSpec(memory_space=pltpu.VMEM),
        scratch_shapes=[pltpu.VMEM(keys.shape, keys.dtype)] * 2 + [pltpu.SemaphoreType.DMA((2,))],
        compiler_params=pltpu.CompilerParams(vmem_limit_bytes=60 * 1024 * 1024),
        name="pack",
    )(keys, values)


def swapped(value):
    return lax.ppermute(value, "core", [(0, 1), (1, 0)])


def shifted(value, shift):
    size = lax.axis_size("x")
    return lax.ppermute(value, "x", [(i, (i + shift) % size) for i in range(size)])


def exchanged(blocks):
    return lax.all_to_all(blocks, HEAD_AXES, 0, 0, tiled=True)


def attention(queries, key_vectors, value_vectors, noise_levels, visible, level_gates):
    groups = visible.shape[0]
    pair = exchanged(packed(key_vectors, value_vectors))
    key = pair[:, 0].reshape(groups, -1, HEAD_DIM)
    value = pair[:, 1].reshape(groups, -1, HEAD_DIM)
    query = exchanged(to_heads(queries)).reshape(groups, -1, HEAD_DIM)
    key_up, key_down = shifted(key, 1), shifted(key, -1)
    value_up, value_down = shifted(value, 1), shifted(value, -1)
    key_far, value_far = shifted(key_up, 1), shifted(value_down, -1)
    lists = live_pairs(visible)
    head = lax.axis_index(HEAD_AXES)
    gates = lax.dynamic_slice_in_dim(level_gates, head * HEAD_DIM, HEAD_DIM, axis=1)
    lists, gates = lax.optimization_barrier((lists, gates))
    early = [key, value, key_up, value_up]
    early += [swapped(piece) for piece in early]
    late = [key_down, value_down]
    late += [swapped(piece) for piece in late]
    state = attend_call(["two"] * 4, True, False, lists, noise_levels, query, early)
    key_far, value_far, top = lax.optimization_barrier((key_far, value_far, state[0]))
    late += [key_far, value_far, swapped(key_far), swapped(value_far)]
    late += [top, *state[1:], gates]
    out = attend_call(["two"] * 4, False, True, lists, noise_levels, query, late)
    back = out.reshape(lax.axis_size(HEAD_AXES), -1, HEAD_DIM)
    back = lax.all_to_all(back, HEAD_AXES, 0, 0, tiled=True)
    return back.transpose(1, 0, 2).reshape(queries.shape)


def solution(mesh):
    split = Mesh(mesh.devices.reshape(8, 2, 2, 4, 2), AXES)
    rows = P(AXES, None)
    return jax.shard_map(
        attention,
        mesh=split,
        in_specs=(rows, rows, rows, P(), P(), P()),
        out_specs=rows,
        check_vma=False,
    )
```

```python
import functools
import math

import jax
import jax.numpy as jnp
from jax import lax
from jax.experimental import pallas as pl
from jax.experimental.pallas import tpu as pltpu
from jax.sharding import Mesh
from jax.sharding import PartitionSpec as P


HEAD_DIM = 128
AXES = ("z", "yh", "yl", "x", "core")
HEAD_AXES = ("z", "yh", "yl")
NEGATIVE = -1e30
UNROLL = 9
TO_EXP2 = math.log2(math.e) / math.sqrt(HEAD_DIM)


def attend(sources, first, last, groups, lists, q_ref, *refs):
    refs = list(refs)
    keys, values = [], []
    for kind in sources:
        if kind == "pair":
            ref = refs.pop(0)
            keys.append(ref.at[0])
            values.append(ref.at[1])
        else:
            keys.append(refs.pop(0))
            values.append(refs.pop(0))
    if not first:
        old_m, old_l, old_acc = refs[:3]
        refs = refs[3:]
    if last:
        gate_ref, o_ref, m_ref, l_ref, acc_ref, turned_ref, padded_ref, *scores_ref, done = refs
    else:
        m_ref, l_ref, acc_out, acc_ref, turned_ref, padded_ref, *scores_ref, done = refs
    if first:
        m_ref[...] = jnp.full_like(m_ref, NEGATIVE)
        l_ref[...] = jnp.zeros_like(l_ref)
        acc_ref[...] = jnp.zeros_like(acc_ref)
    else:
        m_ref[...] = old_m[...]
        l_ref[...] = old_l[...]
        fetch = pltpu.make_async_copy(old_acc.at[: groups + 1], acc_ref, done)
        fetch.start()

    pad = HEAD_DIM - q_ref.shape[1]

    def prepare(c, carry):
        turned_ref[c] = jnp.concatenate([v[c] for v in values], axis=0).T
        padded_ref[c] = jnp.concatenate([q_ref[c], jnp.zeros((pad, HEAD_DIM), q_ref.dtype)], axis=0)
        return carry

    lax.fori_loop(0, groups, prepare, 0, unroll=4)

    def scores(i, score_ref):
        block = jnp.concatenate([k[lists[2, i]] for k in keys], axis=0)
        query = jnp.concatenate([padded_ref[lists[0, i]], padded_ref[lists[1, i]]], axis=0)
        score_ref[...] = lax.dot_general(
            block, query, (((1,), (1,)), ((), ())), preferred_element_type=jnp.float32
        )

    def weigh(i, u):
        score = scores_ref[u]
        high = jnp.max(score[...], axis=0, keepdims=True)
        weight = jnp.exp2((score[...] - high) * TO_EXP2)
        total = jnp.sum(weight, axis=0, keepdims=True)
        update = jnp.dot(
            turned_ref[lists[2, i]], weight.astype(jnp.bfloat16), preferred_element_type=jnp.float32
        )
        return high, total, update

    def merge(i, found):
        high, total, update = found
        for part in range(2):
            slot = lists[3 + part, i]
            lanes = slice(part * HEAD_DIM, (part + 1) * HEAD_DIM)
            old = m_ref[slot]
            new = jnp.maximum(old, high[:, lanes])
            keep = jnp.exp2((old - new) * TO_EXP2)
            take = jnp.exp2((high[:, lanes] - new) * TO_EXP2)
            m_ref[slot] = new
            l_ref[slot] = l_ref[slot] * keep + total[:, lanes] * take
            acc_ref[slot] = acc_ref[slot] * keep + update[:, lanes] * take

    for u in range(UNROLL):
        scores(u, scores_ref[u])

    def step(j, carry):
        found = []
        for u in range(UNROLL):
            found.append(weigh(UNROLL * j + u, u))
            scores(UNROLL * (j + 1) + u, scores_ref[u])
        for u in range(UNROLL):
            merge(UNROLL * j + u, found[u])
        return carry

    if not first:
        fetch.wait()

    lax.fori_loop(0, lists[5, 0], step, 0)

    if not last:
        store = pltpu.make_async_copy(acc_ref, acc_out.at[: groups + 1], done)
        store.start()
        store.wait()

    if last:

        def finish(c, carry):
            gate = gate_ref[pl.ds(lists[6, c], 1), :]
            ratio = (acc_ref[c] / l_ref[c]).T[: q_ref.shape[1]]
            o_ref[c] = (ratio * gate).astype(o_ref.dtype)
            return carry

        lax.fori_loop(0, groups, finish, 0, unroll=4)


def attend_call(sources, first, last, lists, query, operands):
    groups, rows, _ = query.shape
    width = len(sources) * rows
    blocks = groups * (groups + 1) // 2
    vmem = pl.BlockSpec(memory_space=pltpu.VMEM)
    smem = pl.BlockSpec(memory_space=pltpu.SMEM)
    state = [(groups + 1, 1, HEAD_DIM), (groups + 1, 1, HEAD_DIM), (groups + 1, HEAD_DIM, HEAD_DIM)]
    work = [
        pltpu.VMEM((groups, HEAD_DIM, width), jnp.bfloat16),
        pltpu.VMEM((groups, HEAD_DIM, HEAD_DIM), jnp.bfloat16),
    ] + [pltpu.VMEM((width, 2 * HEAD_DIM), jnp.float32)] * UNROLL
    if last:
        out_shape = jax.ShapeDtypeStruct(query.shape, jnp.bfloat16)
        scratch = [pltpu.VMEM(shape, jnp.float32) for shape in state] + work
        out_specs = vmem
    else:
        roomy = (8 * (groups + 1), *state[2][1:])
        out_shape = [jax.ShapeDtypeStruct(shape, jnp.float32) for shape in (*state[:2], roomy)]
        scratch = [pltpu.VMEM(state[2], jnp.float32)] + work
        out_specs = [vmem, vmem, pl.BlockSpec(memory_space=pltpu.HBM)]
    in_specs = [smem] + [vmem] * (1 + len(operands))
    if not first:
        in_specs[-2 if last else -1] = pl.BlockSpec(memory_space=pltpu.HBM)
    return pl.pallas_call(
        functools.partial(attend, sources, first, last, groups),
        out_shape=out_shape,
        in_specs=in_specs,
        out_specs=out_specs,
        scratch_shapes=scratch + [pltpu.SemaphoreType.DMA],
        compiler_params=pltpu.CompilerParams(vmem_limit_bytes=16 * 1024 * 1024),
        cost_estimate=pl.CostEstimate(
            flops=12 * blocks * rows * width * HEAD_DIM,
            bytes_accessed=4 * len(sources) * query.size,
            transcendentals=blocks * rows * width,
        ),
        name="attend_last" if last else "attend_first",
    )(lists, query, *operands)


def live_pairs(visible, noise_levels):
    groups = visible.shape[0]
    ids = jnp.arange(groups, dtype=jnp.int32)
    c, e = ids[:, None], ids[None, :]
    live = (c == e) | (e < c) & (visible == 1)
    rank = jnp.sum((live[None, :, :] & (ids[None, :] < ids[:, None])[:, :, None]).astype(jnp.int32), axis=1)
    seen = jnp.sum(live.astype(jnp.int32), axis=0)
    pairs = (seen + 1) // 2
    start = jnp.sum(jnp.where(ids[None, :] < ids[:, None], pairs[None, :], 0), axis=1)
    total = jnp.sum(pairs)
    length = sum((n + 1) // 2 for n in range(1, groups + 1)) + 2 * UNROLL - 1
    places = jnp.arange(length, dtype=jnp.int32)
    column = start[None, :] + rank // 2
    rows = []
    for part in range(2):
        here = live & (rank % 2 == part)
        taken = here[None, :, :] & (column[None, :, :] == places[:, None, None])
        found = jnp.any(taken, axis=(1, 2))
        query = jnp.sum(jnp.where(taken, ids[None, :, None], 0), axis=(1, 2))
        key = jnp.sum(jnp.where(taken, ids[None, None, :], 0), axis=(1, 2))
        rows.append((query, key, jnp.where(found, query, groups)))
    (q0, key, s0), (q1, _, s1) = rows
    steps = jnp.broadcast_to((total + UNROLL - 1) // UNROLL, places.shape)
    noise = jnp.pad(noise_levels, (0, length - groups))
    return jnp.stack([q0, q1, key, s0, s1, steps, noise])


def to_heads(value):
    return value.reshape(value.shape[0], -1, HEAD_DIM).transpose(1, 0, 2)


def pack(k_hbm, v_hbm, o_ref, k_ref, v_ref, done):
    fetches = [pltpu.make_async_copy(k_hbm, k_ref, done.at[0]), pltpu.make_async_copy(v_hbm, v_ref, done.at[1])]
    for fetch in fetches:
        fetch.start()
    for i, ref in enumerate((k_ref, v_ref)):
        fetches[i].wait()
        for h in range(o_ref.shape[0]):
            o_ref[h, i] = ref[:, h * HEAD_DIM : (h + 1) * HEAD_DIM]


def packed(keys, values):
    tokens, width = keys.shape
    hbm = pl.BlockSpec(memory_space=pltpu.HBM)
    return pl.pallas_call(
        pack,
        out_shape=jax.ShapeDtypeStruct((width // HEAD_DIM, 2, tokens, HEAD_DIM), keys.dtype),
        in_specs=[hbm, hbm],
        out_specs=pl.BlockSpec(memory_space=pltpu.VMEM),
        scratch_shapes=[pltpu.VMEM(keys.shape, keys.dtype)] * 2 + [pltpu.SemaphoreType.DMA((2,))],
        compiler_params=pltpu.CompilerParams(vmem_limit_bytes=60 * 1024 * 1024),
        name="pack",
    )(keys, values)


def swapped(value):
    return lax.ppermute(value, "core", [(0, 1), (1, 0)])


def shifted(value, shift):
    size = lax.axis_size("x")
    return lax.ppermute(value, "x", [(i, (i + shift) % size) for i in range(size)])


def exchanged(blocks):
    return lax.all_to_all(blocks, HEAD_AXES, 0, 0, tiled=True)


def attention(queries, key_vectors, value_vectors, noise_levels, visible, level_gates):
    groups = visible.shape[0]
    pair = exchanged(packed(key_vectors, value_vectors))
    key = pair[:, 0].reshape(groups, -1, HEAD_DIM)
    value = pair[:, 1].reshape(groups, -1, HEAD_DIM)
    lists = live_pairs(visible, noise_levels)
    head = lax.axis_index(HEAD_AXES)
    gates = lax.dynamic_slice_in_dim(level_gates, head * HEAD_DIM, HEAD_DIM, axis=1)
    blocks, lists, gates = lax.optimization_barrier((to_heads(queries), lists, gates))
    query = exchanged(blocks).reshape(groups, -1, HEAD_DIM)
    key_up, key_down = shifted(key, 1), shifted(key, -1)
    value_up, value_down = shifted(value, 1), shifted(value, -1)
    key_far, value_far = shifted(key_up, 1), shifted(value_down, -1)
    early = [key, value, key_up, value_up]
    early += [swapped(piece) for piece in early]
    late = [key_down, value_down]
    late += [swapped(piece) for piece in late]
    state = attend_call(["two"] * 4, True, False, lists, query, early)
    key_far, value_far, top = lax.optimization_barrier((key_far, value_far, state[0]))
    late += [key_far, value_far, swapped(key_far), swapped(value_far)]
    late += [top, *state[1:], gates]
    out = attend_call(["two"] * 4, False, True, lists, query, late)
    back = out.reshape(lax.axis_size(HEAD_AXES), -1, HEAD_DIM)
    back = lax.all_to_all(back, HEAD_AXES, 0, 0, tiled=True)
    return back.transpose(1, 0, 2).reshape(queries.shape)


def solution(mesh):
    split = Mesh(mesh.devices.reshape(8, 2, 2, 4, 2), AXES)
    rows = P(AXES, None)
    return jax.shard_map(
        attention,
        mesh=split,
        in_specs=(rows, rows, rows, P(), P(), P()),
        out_specs=rows,
        check_vma=False,
    )
```
